1024 devices in a mesh: tensor: 32 (over z_hi, y, core), context: 32 (over z_lo, x).
Axes of the slice: x: 4, y: 4, z: 32 (z_hi: 4, z_lo: 8; z = z_hi * 8 + z_lo), core: 2. Of those that a mesh axis runs over, the one named last changes fastest.
Arguments:
- query_rows: bfloat16 [8192, 8192], P('context', 'tensor'), may hold values from -160 to 160, as said below
- key_rows: bfloat16 [8192, 1024], P('context'), may hold values from -5 to 5, as said below
- value_rows: bfloat16 [8192, 1024], P('context'), may hold values from -6 to 6
- doc_ids: int32 [8192], P('context'), may hold values from 0 to 15, never falling along the last dimension, each value on 1 to 1024 neighbouring positions
- out_weight: bfloat16 [8192, 8192], P('tensor'), may hold values from -0.125 to 0.125
Outputs:
- mixed: bfloat16 [8192, 8192], P('context', 'tensor')
The draws below stay inside these ranges and needn't reach their ends.
Inputs may be any that keep to these rules, and one draw needn't show every extreme that they name: `query_rows`: within the range given by the table of arrays. `key_rows`: within the range given by the table of arrays. `doc_ids`: document numbers never fall along the sequence; every document has 1 to 1024 tokens and one has exactly 1024.
All inputs are finite; a program needn't handle non-finite values.
Results may differ from the reference program's by a relative error of at most 0.015.
Values may be sent and summed in bfloat16 or wider, within the bound.
A program may use at most 64 MiB of HBM per device.

```python
import math
import jax
import jax.numpy as jnp
import numpy as np
from jax import lax

D = 8192
H = 64
KVH = 8
HD = 128
TOK_DEV = 256
DOC_MOST = 1024
TOKENS = 8192
DOCS = 16
N_TENSOR = 32


def make_pairs(key):
    key_draw = jnp.clip(jax.random.normal(jax.random.fold_in(key, 101), (TOKENS, KVH, HD), jnp.float32), -5.0, 5.0)
    query_draw = jax.random.normal(jax.random.fold_in(key, 202), (TOKENS, H, HD), jnp.float32)
    return (query_draw.reshape(TOKENS, H * HD), key_draw.reshape(TOKENS, KVH * HD))


def draw_query_rows(key, part):
    return make_pairs(key)[0].astype(jnp.bfloat16)


def draw_key_rows(key, part):
    return make_pairs(key)[1].astype(jnp.bfloat16)


def raised(result, own_key, source, target, shards_of, factor):
    def block_of(position):
        return (jnp.arange(result.shape[position]) // (result.shape[position] // shards_of)).reshape((-1,) + (1,) * (result.ndim - 1 - position))

    near = jax.random.permutation(own_key, shards_of)[block_of(target)]
    second = (block_of(target) + shards_of // 2) % shards_of
    return jnp.where((block_of(source) == near) | (block_of(source) == second), factor * result, result)


def shard_levels(rng, shape, split, least, largest):
    def one(axis_at, parts):
        heights = jax.random.uniform(jax.random.fold_in(jax.random.fold_in(rng, 6), axis_at), (parts,), jnp.float32, least / len(split), largest / len(split))
        return jnp.repeat(jnp.exp(heights), shape[axis_at] // parts).reshape((-1,) + (1,) * (len(shape) - axis_at - 1))

    gain = one(*split[0])
    for cut in split[1:]:
        gain = gain * one(*cut)
    return gain


def profile(amount, total, reach, lean):
    portions = [(1 << 20) // math.isqrt(standing ** lean) + 1 for standing in range(2, amount + 1)]
    spare, holding = total - reach - (amount - 1), [1] * (amount - 1)
    while spare > 0:
        candidates = [i for i in range(amount - 1) if holding[i] < reach]
        mass, left = sum([portions[i] for i in candidates]), spare
        for i in candidates:
            extra = min(reach - holding[i], max(1, left * portions[i] // mass), spare)
            holding[i] = holding[i] + extra
            spare = spare - extra
    return np.array([reach] + holding)


def ragged(own_key, number_of, total, limit, lean):
    if number_of == 2:
        one = jax.random.randint(own_key, (), max(1, total - limit), min(limit, total - 1) + 1)
        return jnp.stack([one, total - one])
    lengths = jnp.asarray(profile(number_of, total, limit, lean), jnp.int32)
    twos = (number_of - 1) // 2
    source_of, receiver = lengths[1:1 + 2 * twos:2], lengths[2:2 + 2 * twos:2]
    slack = jnp.minimum(source_of - 1, limit - receiver)
    shifted = jax.random.randint(jax.random.fold_in(own_key, 1), (twos,), 0, 1 << 20) % (slack + 1)
    lengths = lengths.at[1:1 + 2 * twos:2].set(source_of - shifted).at[2:2 + 2 * twos:2].set(receiver + shifted)
    return lengths[jax.random.permutation(jax.random.fold_in(own_key, 2), number_of)]


def normal_values(rng, shape, deviation, limit, cuts=(), kind=jnp.bfloat16):
    values = jax.random.normal(rng, shape, jnp.float32) * deviation
    if len(cuts) > 0:
        values = shard_levels(rng, shape, cuts, -0.22, 0.18) * values
    return jnp.clip(values, min=-limit, max=limit).astype(kind)


def bell_draw_with(stream_key, extent, width, most, cuts, heavy, kind=jnp.bfloat16):
    values = width * jax.random.normal(stream_key, extent, jnp.float32)
    if cuts:
        values = values * shard_levels(stream_key, extent, cuts, -0.22, 0.18)
    return jnp.clip(raised(values, jax.random.fold_in(stream_key, 3), *heavy), -most, most).astype(kind)


def setup_inputs(seed: int = 0) -> dict:
    key_of = jax.random.split(jax.random.key(seed), 6)
    return {
        "query_rows": draw_query_rows(jax.random.fold_in(key_of[5], 71), 0),
        "key_rows": draw_key_rows(jax.random.fold_in(key_of[5], 71), 0),
        "value_rows": normal_values(key_of[2], (TOKENS, KVH * HD), 1.0, 6.0, ((0, 32),)),
        "doc_ids": jnp.searchsorted(jnp.cumsum(ragged(key_of[3], DOCS, TOKENS, DOC_MOST, 2)), jnp.arange(TOKENS), side="right").astype(jnp.int32),
        "out_weight": bell_draw_with(key_of[4], (H * HD, D), (H * HD) ** -0.5, 0.125, ((0, 32),), (0, 1, 32, 2.75)),
    }


def reference(query_rows, key_rows, value_rows, doc_ids, out_weight):
    group_size = H // KVH
    key_span = DOC_MOST + TOK_DEV
    padded_keys = jnp.pad(key_rows, ((DOC_MOST, 0), (0, 0)))
    padded_values = jnp.pad(value_rows, ((DOC_MOST, 0), (0, 0)))
    padded_docs = jnp.pad(doc_ids, (DOC_MOST, 0), constant_values=-1)

    def one_block(block_index):
        first_row = (block_index * TOK_DEV).astype(jnp.int32)
        block_queries = lax.dynamic_slice_in_dim(query_rows, first_row, TOK_DEV, 0)
        block_queries = block_queries.astype(jnp.float32).reshape(TOK_DEV, KVH, group_size, HD)
        window_keys = lax.dynamic_slice_in_dim(padded_keys, first_row, key_span, 0)
        window_keys = window_keys.astype(jnp.float32).reshape(key_span, KVH, HD)
        window_values = lax.dynamic_slice_in_dim(padded_values, first_row, key_span, 0)
        window_values = window_values.astype(jnp.float32).reshape(key_span, KVH, HD)
        window_docs = lax.dynamic_slice_in_dim(padded_docs, first_row, key_span, 0)
        query_docs = lax.dynamic_slice_in_dim(doc_ids, first_row, TOK_DEV, 0)
        query_pos = first_row + jnp.arange(TOK_DEV, dtype=jnp.int32)
        key_pos = first_row - DOC_MOST + jnp.arange(key_span, dtype=jnp.int32)
        allowed = (key_pos[None, :] <= query_pos[:, None]) & (window_docs[None, :] == query_docs[:, None])
        scores = jnp.einsum("tkgd,skd->kgts", block_queries, window_keys) * (HD ** -0.5)
        scores = jnp.where(allowed, scores, -jnp.inf)
        highest = jnp.max(scores, axis=-1, keepdims=True)
        weights = jnp.where(allowed, jnp.exp(scores - highest), 0.0)
        totals = jnp.sum(weights, axis=-1)
        rounded = lax.optimization_barrier(weights.astype(jnp.bfloat16)).astype(jnp.float32)
        numer = jnp.einsum("kgts,skd->kgtd", rounded, window_values)
        attended = numer / totals[..., None]
        return attended.transpose(2, 0, 1, 3).reshape(TOK_DEV, H * HD).astype(jnp.bfloat16)

    blocks = lax.map(one_block, jnp.arange(TOKENS // TOK_DEV, dtype=jnp.int32))
    attended = blocks.reshape(TOKENS, H * HD)
    local_width = (H // N_TENSOR) * HD

    def add_group(index, running):
        first_col = (index * local_width).astype(jnp.int32)
        columns = lax.dynamic_slice_in_dim(attended, first_col, local_width, 1)
        weight_rows = lax.dynamic_slice_in_dim(out_weight, first_col, local_width, 0)
        partial_value = jnp.dot(columns, weight_rows, preferred_element_type=jnp.float32)
        rounded = lax.optimization_barrier(partial_value.astype(jnp.bfloat16)).astype(jnp.float32)
        return running + rounded

    mixed = lax.fori_loop(0, N_TENSOR, add_group, jnp.zeros((TOKENS, D), jnp.float32))
    return mixed.astype(jnp.bfloat16)
```

```python
import jax
import jax.numpy as jnp
from jax import lax
from jax.experimental import pallas as pl
from jax.experimental.pallas import tpu as pltpu
from jax.sharding import PartitionSpec as P

HD = 128
GROUP = 8
BACK = 4
TOK = 256
HALF = TOK // 2
NEG_BIG = -1e30
SCALE = HD**-0.5 * 1.4426950408889634
MESH = pl.DeviceIdType.MESH
OFFSETS = (2, 1, 3, 0)
BLOCKS = BACK + 1
KEYS = BLOCKS * TOK


def kernel(
    n_ctx,
    q_ref,
    k_ref,
    v_ref,
    doc_ref,
    w_ref,
    out_ref,
    kv,
    docs,
    dq,
    s_buf,
    m_buf,
    p_buf,
    l_buf,
    a_buf,
    w_buf,
    p_out,
    y_in,
    z_out,
    z_in,
    loc_sem,
    w_sem,
    wx_send,
    wx_recv,
    kv_send,
    kv_recv,
    doc_send,
    doc_recv,
    fwd_send,
    fwd_recv,
    a_send,
    a_recv,
    y_send,
    y_recv,
    z_send,
    z_recv,
):
    c = lax.axis_index("context")
    t = lax.axis_index("tensor")
    core = lax.rem(t, 2)
    y = lax.rem(t // 2, 4)
    z = t // 8
    other = 1 - core

    def dev(dz, dy, same_core=True):
        who = core if same_core else other
        return {"tensor": (lax.rem(z + dz, 4) * 4 + lax.rem(y + dy, 4)) * 2 + who}

    barrier = pltpu.get_barrier_semaphore()
    for where in (dev(0, 0, False), dev(0, 1), dev(0, 3), dev(1, 0), dev(3, 0)):
        pl.semaphore_signal(barrier, inc=1, device_id=where, device_id_type=MESH)
    for k in range(1, BACK + 1):

        @pl.when(c + k < n_ctx)
        def _():
            pl.semaphore_signal(
                barrier, inc=1, device_id={"context": c + k}, device_id_type=MESH
            )

        @pl.when(c >= k)
        def _():
            pl.semaphore_signal(
                barrier, inc=1, device_id={"context": c - k}, device_id_type=MESH
            )

    head = pl.multiple_of((t // 4) * HD, HD)
    k_copy = pltpu.make_async_copy(
        k_ref.at[:, pl.ds(head, HD)], kv.at[0, pl.ds(0, TOK), :], loc_sem.at[0]
    )
    v_copy = pltpu.make_async_copy(
        v_ref.at[:, pl.ds(head, HD)], kv.at[1, pl.ds(0, TOK), :], loc_sem.at[1]
    )
    k_copy.start()
    v_copy.start()

    def columns(r, q, who):
        j = lax.rem(z + OFFSETS[r], 4) * 4 + lax.rem(y + OFFSETS[q], 4)
        return pl.ds(pl.multiple_of((j * 2 + who) * TOK, TOK), TOK)

    def w_local(r, q):
        i = r * 4 + q
        return pltpu.make_async_copy(
            w_ref.at[:, columns(r, q, core)], w_buf.at[i, core], w_sem.at[i]
        )

    def w_cross(r, q):
        i = r * 4 + q
        return pltpu.make_async_remote_copy(
            src_ref=w_ref.at[:, columns(r, q, other)],
            dst_ref=w_buf.at[i, core],
            send_sem=wx_send.at[i],
            recv_sem=wx_recv.at[i],
            device_id=dev(0, 0, False),
            device_id_type=MESH,
        )

    def w_cross_in(r, q):
        i = r * 4 + q
        return pltpu.make_async_remote_copy(
            src_ref=w_ref.at[:, columns(r, q, other)],
            dst_ref=w_buf.at[i, other],
            send_sem=wx_send.at[i],
            recv_sem=wx_recv.at[i],
            device_id=dev(0, 0, False),
            device_id_type=MESH,
        )

    for r in range(4):
        for q in range(4):
            w_local(r, q).start()

    row = doc_ref[...]
    docs[0] = jnp.broadcast_to(row, (8, TOK))
    dq[...] = jnp.broadcast_to(row, (TOK, TOK)).T
    for k in range(1, BACK + 1):

        @pl.when(c < k)
        def _():
            kv[:, pl.ds(k * TOK, TOK), :] = jnp.zeros((2, TOK, HD), jnp.bfloat16)
            docs[k] = jnp.full((8, TOK), -1, jnp.int32)

    k_copy.wait()
    v_copy.wait()
    partners = 5 + jnp.minimum(c, BACK) + jnp.minimum(n_ctx - 1 - c, BACK)
    pl.semaphore_wait(barrier, partners)

    def kv_out(k):
        return pltpu.make_async_remote_copy(
            src_ref=kv.at[core, pl.ds(0, TOK), :],
            dst_ref=kv.at[core, pl.ds(k * TOK, TOK), :],
            send_sem=kv_send.at[k - 1],
            recv_sem=kv_recv.at[k - 1],
            device_id={"context": c + k},
            device_id_type=MESH,
        )

    def doc_out(k):
        return pltpu.make_async_remote_copy(
            src_ref=docs.at[0],
            dst_ref=docs.at[k],
            send_sem=doc_send.at[k - 1],
            recv_sem=doc_recv.at[k - 1],
            device_id={"context": c + k},
            device_id_type=MESH,
        )

    def forward(k, who):
        return pltpu.make_async_remote_copy(
            src_ref=kv.at[who, pl.ds(k * TOK, TOK), :],
            dst_ref=kv.at[who, pl.ds(k * TOK, TOK), :],
            send_sem=fwd_send.at[k - 1],
            recv_sem=fwd_recv.at[k - 1],
            device_id=dev(0, 0, False),
            device_id_type=MESH,
        )

    for k in range(1, BACK + 1):

        @pl.when(c + k < n_ctx)
        def _():
            doc_out(k).start()
            kv_out(k).start()

    for r in range(4):
        for q in range(4):
            w_cross(r, q).start()

    def scores(k):
        keys = kv[0, pl.ds(k * TOK, TOK), :]
        mask = dq[...] == docs[k, 0:1, :]
        if k == 0:
            i = lax.broadcasted_iota(jnp.int32, (TOK, TOK), 0)
            j = lax.broadcasted_iota(jnp.int32, (TOK, TOK), 1)
            mask = mask & (j <= i)
        for h in range(2):
            s = lax.dot_general(
                q_ref[:, pl.ds(h * HD, HD)],
                keys,
                (((1,), (1,)), ((), ())),
                preferred_element_type=jnp.float32,
            )
            s = jnp.where(mask, s * SCALE, NEG_BIG)
            rows = pl.ds(h * TOK, TOK)
            s_buf[k, rows, :] = s
            if k == 0:
                m_buf[rows, :] = s
            else:
                m_buf[rows, :] = jnp.maximum(m_buf[rows, :], s)

    scores(0)
    for k in range(1, BACK + 1):

        @pl.when(c >= k)
        def _():
            kv_out(k).wait_recv()
            forward(k, core).start()

        if k >= 2:

            @pl.when(c >= k - 1)
            def _():
                forward(k - 1, other).wait_recv()
                doc_out(k - 1).wait_recv()

            scores(k - 1)

    @pl.when(c >= BACK)
    def _():
        forward(BACK, other).wait_recv()
        doc_out(BACK).wait_recv()

    scores(BACK)

    def softmax(i, carry):
        rows = pl.ds(pl.multiple_of(i * 64, 64), 64)
        top = jnp.max(m_buf[rows, :], axis=-1, keepdims=True)
        total = jnp.zeros((64, TOK), jnp.float32)
        for k in range(BLOCKS):
            e = jnp.exp2(s_buf[k, rows, :] - top)
            total = total + e
            p_buf[rows, pl.ds(k * TOK, TOK)] = e.astype(jnp.bfloat16)
        l_buf[rows, :] = jnp.broadcast_to(jnp.sum(total, axis=-1, keepdims=True), (64, HD))
        return carry

    lax.fori_loop(0, 8, softmax, 0)
    for h in range(2):
        rows = pl.ds(h * TOK, TOK)
        o = jnp.dot(p_buf[rows, :], kv[1], preferred_element_type=jnp.float32)
        a_buf[core, :, pl.ds(h * HD, HD)] = (o / l_buf[rows, :]).astype(jnp.bfloat16)

    def a_copy(who):
        return pltpu.make_async_remote_copy(
            src_ref=a_buf.at[who],
            dst_ref=a_buf.at[who],
            send_sem=a_send.at[0],
            recv_sem=a_recv.at[0],
            device_id=dev(0, 0, False),
            device_id_type=MESH,
        )

    a_copy(core).start()
    for r in range(4):
        for q in range(4):
            w_local(r, q).wait()
            w_cross_in(r, q).wait_recv()
    a_copy(other).wait_recv()

    lo, hi = pl.ds(0, HALF), pl.ds(HALF, HALF)

    def project(r, q):
        i = r * 4 + q
        p = jnp.dot(a_buf[0], w_buf[i, 0], preferred_element_type=jnp.float32)
        p = p + jnp.dot(a_buf[1], w_buf[i, 1], preferred_element_type=jnp.float32)
        p_out[r, q] = p.astype(jnp.bfloat16)

    def y_copy(r, slot, src):
        return pltpu.make_async_remote_copy(
            src_ref=src,
            dst_ref=y_in.at[r, slot],
            send_sem=y_send.at[r, slot],
            recv_sem=y_recv.at[r, slot],
            device_id=dev(0, 1 if slot % 2 == 0 else 3),
            device_id_type=MESH,
        )

    def y_src(r, slot):
        q, half = ((0, lo), (0, hi), (1, hi), (2, lo), (1, lo), (2, hi))[slot]
        return p_out.at[r, q, half, :]

    def y_start(r, slot):
        y_copy(r, slot, y_src(r, slot)).start()

    def y_got(r, slot):
        y_copy(r, slot, y_src(r, slot)).wait_recv()
        return y_in[r, slot].astype(jnp.float32)

    def stage_a(r):
        project(r, 0)
        y_start(r, 0)
        y_start(r, 1)

    def stage_d(r):
        project(r, 1)
        y_start(r, 2)
        project(r, 2)
        y_start(r, 3)
        project(r, 3)

    def stage_b(r):
        up = p_out[r, 1, lo, :].astype(jnp.float32) + y_got(r, 0)
        p_out[r, 1, lo, :] = up.astype(jnp.bfloat16)
        y_start(r, 4)
        down = p_out[r, 2, hi, :].astype(jnp.float32) + y_got(r, 1)
        p_out[r, 2, hi, :] = down.astype(jnp.bfloat16)
        y_start(r, 5)

    def y_sum(r):
        low = p_out[r, 3, lo, :].astype(jnp.float32) + y_got(r, 3) + y_got(r, 4)
        high = p_out[r, 3, hi, :].astype(jnp.float32) + y_got(r, 2) + y_got(r, 5)
        return low, high

    def z_copy(slot):
        r, half = ((0, lo), (0, hi), (1, hi), (2, lo), (1, lo), (2, hi))[slot]
        return pltpu.make_async_remote_copy(
            src_ref=z_out.at[r, half, :],
            dst_ref=z_in.at[slot],
            send_sem=z_send.at[slot],
            recv_sem=z_recv.at[slot],
            device_id=dev(1 if slot % 2 == 0 else 3, 0),
            device_id_type=MESH,
        )

    def z_got(slot):
        z_copy(slot).wait_recv()
        return z_in[slot].astype(jnp.float32)

    def y_done(r):
        low, high = y_sum(r)
        z_out[r, lo, :] = low.astype(jnp.bfloat16)
        z_out[r, hi, :] = high.astype(jnp.bfloat16)
        if r == 0:
            z_copy(0).start()
            z_copy(1).start()
        elif r == 1:
            z_copy(2).start()
        else:
            z_copy(3).start()

    stage_a(0)
    stage_d(0)
    stage_a(1)
    stage_b(0)
    stage_d(1)
    stage_a(2)
    stage_b(1)
    stage_d(2)
    stage_a(3)
    y_done(0)
    stage_b(2)
    stage_d(3)
    y_done(1)
    stage_b(3)
    y_done(2)
    own_low, own_high = y_sum(3)
    up = z_out[1, lo, :].astype(jnp.float32) + z_got(0)
    z_out[1, lo, :] = up.astype(jnp.bfloat16)
    z_copy(4).start()
    down = z_out[2, hi, :].astype(jnp.float32) + z_got(1)
    z_out[2, hi, :] = down.astype(jnp.bfloat16)
    z_copy(5).start()
    own_low = own_low + z_got(3)
    own_high = own_high + z_got(2)
    out_ref[lo, :] = (own_low + z_got(4)).astype(jnp.bfloat16)
    out_ref[hi, :] = (own_high + z_got(5)).astype(jnp.bfloat16)

    for k in range(1, BACK + 1):

        @pl.when(c + k < n_ctx)
        def _():
            doc_out(k).wait_send()
            kv_out(k).wait_send()

        @pl.when(c >= k)
        def _():
            forward(k, core).wait_send()

    a_copy(core).wait_send()
    for r in range(4):
        for q in range(4):
            w_cross(r, q).wait_send()
        for slot in range(6):
            y_copy(r, slot, y_src(r, slot)).wait_send()
    for slot in range(6):
        z_copy(slot).wait_send()


def solution(mesh):
    n_ctx = mesh.shape["context"]

    def body(query_rows, key_rows, value_rows, doc_ids, out_weight):
        dma = pltpu.SemaphoreType.DMA
        bf16, f32 = jnp.bfloat16, jnp.float32
        vmem = pl.BlockSpec(memory_space=pltpu.VMEM)
        hbm = pl.BlockSpec(memory_space=pltpu.HBM)

        def run(*refs):
            kernel(n_ctx, *refs)

        return pl.pallas_call(
            run,
            out_shape=jax.ShapeDtypeStruct((TOK, TOK), bf16),
            in_specs=[vmem, hbm, hbm, vmem, hbm],
            out_specs=vmem,
            scratch_shapes=[
                pltpu.VMEM((2, KEYS, HD), bf16),
                pltpu.VMEM((BLOCKS, 8, TOK), jnp.int32),
                pltpu.VMEM((TOK, TOK), jnp.int32),
                pltpu.VMEM((BLOCKS, 2 * TOK, TOK), f32),
                pltpu.VMEM((2 * TOK, TOK), f32),
                pltpu.VMEM((2 * TOK, KEYS), bf16),
                pltpu.VMEM((2 * TOK, HD), f32),
                pltpu.VMEM((2, TOK, TOK), bf16),
                pltpu.VMEM((16, 2, TOK, TOK), bf16),
                pltpu.VMEM((4, 4, TOK, TOK), bf16),
                pltpu.VMEM((4, 6, HALF, TOK), bf16),
                pltpu.VMEM((3, TOK, TOK), bf16),
                pltpu.VMEM((6, HALF, TOK), bf16),
                dma((2,)),
                dma((16,)),
                dma((16,)),
                dma((16,)),
                dma((BACK,)),
                dma((BACK,)),
                dma((BACK,)),
                dma((BACK,)),
                dma((BACK,)),
                dma((BACK,)),
                dma((1,)),
                dma((1,)),
                dma((4, 6)),
                dma((4, 6)),
                dma((6,)),
                dma((6,)),
            ],
            compiler_params=pltpu.CompilerParams(
                collective_id=0, has_side_effects=True, vmem_limit_bytes=60 * 2**20
            ),
        )(query_rows, key_rows, value_rows, doc_ids.reshape(1, TOK), out_weight)

    placed = (
        P("context", "tensor"),
        P("context", None),
        P("context", None),
        P("context"),
        P("tensor", None),
    )
    return jax.shard_map(
        body, mesh=mesh, in_specs=placed, out_specs=P("context", "tensor"), check_vma=False
    )
```

```python
import jax
import jax.numpy as jnp
from jax import lax
from jax.experimental import pallas as pl
from jax.experimental.pallas import tpu as pltpu
from jax.sharding import PartitionSpec as P

HD = 128
GROUP = 8
BACK = 4
TOK = 256
HALF = TOK // 2
NEG_BIG = -1e30
SCALE = HD**-0.5 * 1.4426950408889634
MESH = pl.DeviceIdType.MESH
OFFSETS = (2, 1, 3, 0)
ORDER = ((1, 2, 3, 0), (0, 3, 2, 1), (0, 1, 3, 2), (0, 1, 2, 3))
PIECES = 4
ROWS = TOK // PIECES
CCW = ((2, 4, 2, 0), (2, 3, 2, 1), (2, 2, 2, 1), (2, 2, 2, 1))
BLOCKS = BACK + 1
KEYS = BLOCKS * TOK


def kernel(
    n_ctx,
    q_ref,
    k_ref,
    v_ref,
    doc_ref,
    w_ref,
    out_ref,
    kv,
    docs,
    dq,
    m_buf,
    l_buf,
    n_buf,
    a_buf,
    w_buf,
    p_out,
    y_in,
    z_out,
    za_in,
    zd_in,
    q_buf,
    doc_buf,
    own,
    relay,
    loc_sem,
    w_sem,
    wx_send,
    wx_recv,
    kv_send,
    kv_recv,
    doc_send,
    doc_recv,
    fwd_send,
    fwd_recv,
    a_send,
    a_recv,
    y_send,
    y_recv,
    za_send,
    za_recv,
    zd_send,
    zd_recv,
):
    c = lax.axis_index("context")
    t = lax.axis_index("tensor")
    core = lax.rem(t, 2)
    y = lax.rem(t // 2, 4)
    z = t // 8
    other = 1 - core
    lo, hi, whole = pl.ds(0, HALF), pl.ds(HALF, HALF), pl.ds(0, TOK)

    def dev(dz, dy, same_core=True):
        who = core if same_core else other
        return {"tensor": (lax.rem(z + dz, 4) * 4 + lax.rem(y + dy, 4)) * 2 + who}

    x, z_lo = lax.rem(c, 4), c // 4

    def up(d):
        at = z_lo + d
        hi_part = lax.rem(z + at // 8, 4)
        return {"context": lax.rem(at, 8) * 4 + x, "tensor": (hi_part * 4 + y) * 2 + core}

    def down(d):
        at = z_lo + 8 - d
        hi_part = lax.rem(z + 3 + at // 8, 4)
        return {"context": lax.rem(at, 8) * 4 + x, "tensor": (hi_part * 4 + y) * 2 + core}

    def tell(i):
        d = (1, 2, 4)[i]
        for way, where in ((1, up(d)), (0, down(d))):
            pl.semaphore_signal(
                relay.at[i, way], inc=1, device_id=where, device_id_type=MESH
            )

    def hear(i):
        pl.semaphore_wait(relay.at[i, 0], 1)
        pl.semaphore_wait(relay.at[i, 1], 1)

    prompt = jnp.logical_or(z >= 2, jnp.logical_and(z == 0, z_lo == 0))

    barrier = pltpu.get_barrier_semaphore()

    @pl.when(z_lo == 7)
    def _():
        pl.semaphore_signal(barrier, inc=1, device_id=up(1), device_id_type=MESH)

    @pl.when(z_lo == 0)
    def _():
        pl.semaphore_signal(barrier, inc=1, device_id=down(1), device_id_type=MESH)

    for where in (dev(0, 0, False), dev(0, 1), dev(0, 3)):
        pl.semaphore_signal(barrier, inc=1, device_id=where, device_id_type=MESH)
    for k in range(1, BACK + 1):

        @pl.when(c + k < n_ctx)
        def _():
            pl.semaphore_signal(
                barrier, inc=1, device_id={"context": c + k}, device_id_type=MESH
            )

        @pl.when(c >= k)
        def _():
            pl.semaphore_signal(
                barrier, inc=1, device_id={"context": c - k}, device_id_type=MESH
            )

    head = pl.multiple_of((t // 4) * HD, HD)
    k_copy = pltpu.make_async_copy(
        k_ref.at[:, pl.ds(head, HD)], kv.at[0, pl.ds(0, TOK), :], loc_sem.at[0]
    )
    v_copy = pltpu.make_async_copy(
        v_ref.at[:, pl.ds(head, HD)], kv.at[1, pl.ds(0, TOK), :], loc_sem.at[1]
    )
    q_copy = pltpu.make_async_copy(q_ref, q_buf, loc_sem.at[2])
    doc_copy = pltpu.make_async_copy(doc_ref, doc_buf, loc_sem.at[3])
    doc_copy.start()
    k_copy.start()
    q_copy.start()
    v_copy.start()

    def columns(r, q, who):
        u = ORDER[3][r]
        for zi in range(3):
            u = jnp.where(z == zi, ORDER[zi][r], u)
        j = u * 4 + lax.rem(y + OFFSETS[q], 4)
        return pl.ds(pl.multiple_of((j * 2 + who) * TOK, TOK), TOK)

    def w_local(r, q):
        i = r * 4 + q
        return pltpu.make_async_copy(
            w_ref.at[:, columns(r, q, core)], w_buf.at[i, core], w_sem.at[i]
        )

    def w_cross(r, q):
        i = r * 4 + q
        return pltpu.make_async_remote_copy(
            src_ref=w_ref.at[:, columns(r, q, other)],
            dst_ref=w_buf.at[i, core],
            send_sem=wx_send.at[i],
            recv_sem=wx_recv.at[i],
            device_id=dev(0, 0, False),
            device_id_type=MESH,
        )

    def w_cross_in(r, q):
        i = r * 4 + q
        return pltpu.make_async_remote_copy(
            src_ref=w_ref.at[:, columns(r, q, other)],
            dst_ref=w_buf.at[i, other],
            send_sem=wx_send.at[i],
            recv_sem=wx_recv.at[i],
            device_id=dev(0, 0, False),
            device_id_type=MESH,
        )

    for r in range(4):
        for q in range(4):
            w_local(r, q).start()

    doc_copy.wait()
    row = doc_buf[...]
    docs[0] = jnp.broadcast_to(row, (8, TOK))
    dq[...] = jnp.broadcast_to(row, (TOK, TOK)).T
    for k in range(1, BACK + 1):

        @pl.when(c < k)
        def _():
            kv[:, pl.ds(k * TOK, TOK), :] = jnp.zeros((2, TOK, HD), jnp.bfloat16)
            docs[k] = jnp.full((8, TOK), -1, jnp.int32)

    def absorb(k, half):
        span = pl.ds(k * TOK, TOK)
        keys, values = kv[0, span, :], kv[1, span, :]
        mask = dq[half, :] == docs[k, 0:1, :]
        if k == 0:
            first = 0 if half is lo else HALF
            i = lax.broadcasted_iota(jnp.int32, (HALF, TOK), 0) + first
            j = lax.broadcasted_iota(jnp.int32, (HALF, TOK), 1)
            mask = mask & (j <= i)
        for h in range(2):
            s = lax.dot_general(
                q_buf[half, pl.ds(h * HD, HD)],
                keys,
                (((1,), (1,)), ((), ())),
                preferred_element_type=jnp.float32,
            )
            s = jnp.where(mask, s * SCALE, NEG_BIG)
            top = jnp.broadcast_to(jnp.max(s, axis=-1, keepdims=True), (HALF, HD))
            if k > 0:
                before = m_buf[h, half, :]
                top = jnp.maximum(before, top)
                keep = jnp.exp2(before - top)
            e = jnp.exp2(s - jnp.concatenate([top, top], axis=1))
            total = jnp.broadcast_to(jnp.sum(e, axis=-1, keepdims=True), (HALF, HD))
            numer = jnp.dot(e.astype(jnp.bfloat16), values, preferred_element_type=jnp.float32)
            if k > 0:
                total = total + keep * l_buf[h, half, :]
                numer = numer + keep * n_buf[h, half, :]
            if k == BACK:
                a_buf[core, half, pl.ds(h * HD, HD)] = (numer / total).astype(jnp.bfloat16)
            else:
                m_buf[h, half, :] = top
                l_buf[h, half, :] = total
                n_buf[h, half, :] = numer

    k_copy.wait()
    q_copy.wait()
    v_copy.wait()
    absorb(0, lo)
    absorb(0, hi)
    partners = 3 + jnp.minimum(c, BACK) + jnp.minimum(n_ctx - 1 - c, BACK)
    partners = partners + jnp.where(z_lo == 0, 1, 0) + jnp.where(z_lo == 7, 1, 0)
    pl.semaphore_wait(barrier, partners)
    tell(0)

    def kv_out(k):
        return pltpu.make_async_remote_copy(
            src_ref=kv.at[core, pl.ds(0, TOK), :],
            dst_ref=kv.at[core, pl.ds(k * TOK, TOK), :],
            send_sem=kv_send.at[k - 1],
            recv_sem=kv_recv.at[k - 1],
            device_id={"context": c + k},
            device_id_type=MESH,
        )

    def doc_out(k):
        return pltpu.make_async_remote_copy(
            src_ref=docs.at[0],
            dst_ref=docs.at[k],
            send_sem=doc_send.at[k - 1],
            recv_sem=doc_recv.at[k - 1],
            device_id={"context": c + k},
            device_id_type=MESH,
        )

    def forward(k, who):
        return pltpu.make_async_remote_copy(
            src_ref=kv.at[who, pl.ds(k * TOK, TOK), :],
            dst_ref=kv.at[who, pl.ds(k * TOK, TOK), :],
            send_sem=fwd_send.at[k - 1],
            recv_sem=fwd_recv.at[k - 1],
            device_id=dev(0, 0, False),
            device_id_type=MESH,
        )

    for k in range(1, BACK + 1):

        @pl.when(c + k < n_ctx)
        def _():
            doc_out(k).start()
            kv_out(k).start()

    for q in range(4):
        w_cross(0, q).start()

    for k in range(1, BACK + 1):

        @pl.when(c >= k)
        def _():
            kv_out(k).wait_recv()
            forward(k, core).start()

        if k == 3:

            @pl.when(prompt)
            def _():
                hear(0)
                tell(1)

        if k >= 2:

            @pl.when(c >= k - 1)
            def _():
                forward(k - 1, other).wait_recv()
                doc_out(k - 1).wait_recv()

            absorb(k - 1, lo)
            absorb(k - 1, hi)

    for r in range(1, 4):
        for q in range(4):
            w_cross(r, q).start()

    @pl.when(prompt)
    def _():
        hear(1)
        tell(2)

    @pl.when(c >= BACK)
    def _():
        forward(BACK, other).wait_recv()
        doc_out(BACK).wait_recv()

    def a_copy(who, half):
        n = 0 if half is lo else 1
        return pltpu.make_async_remote_copy(
            src_ref=a_buf.at[who, half, :],
            dst_ref=a_buf.at[who, half, :],
            send_sem=a_send.at[n],
            recv_sem=a_recv.at[n],
            device_id=dev(0, 0, False),
            device_id_type=MESH,
        )

    for half in (lo, hi):
        absorb(BACK, half)
        a_copy(core, half).start()

    def w_ready(r, q):
        w_local(r, q).wait()
        w_cross_in(r, q).wait_recv()

    def project(r, q, rows):
        i = r * 4 + q
        p = jnp.dot(a_buf[0, rows, :], w_buf[i, 0], preferred_element_type=jnp.float32)
        p = p + jnp.dot(a_buf[1, rows, :], w_buf[i, 1], preferred_element_type=jnp.float32)
        p_out[r, q, rows, :] = p.astype(jnp.bfloat16)

    def y_copy(r, slot, src):
        return pltpu.make_async_remote_copy(
            src_ref=src,
            dst_ref=y_in.at[r, slot],
            send_sem=y_send.at[r, slot],
            recv_sem=y_recv.at[r, slot],
            device_id=dev(0, 1 if slot % 2 == 0 else 3),
            device_id_type=MESH,
        )

    def y_src(r, slot):
        q, half = ((0, lo), (0, hi), (1, hi), (2, lo), (1, lo), (2, hi))[slot]
        return p_out.at[r, q, half, :]

    def y_start(r, slot):
        y_copy(r, slot, y_src(r, slot)).start()

    def y_got(r, slot):
        y_copy(r, slot, y_src(r, slot)).wait_recv()
        return y_in[r, slot].astype(jnp.float32)

    def first_stage():
        for q in range(4):
            w_ready(0, q)
        for half, (slot_a, slot_d, q_d, q_b) in ((lo, (0, 3, 2, 1)), (hi, (1, 2, 1, 2))):
            a_copy(other, half).wait_recv()
            project(0, 0, half)
            y_start(0, slot_a)
            project(0, q_d, half)
            y_start(0, slot_d)
            project(0, q_b, half)
        project(0, 3, whole)

    def stage(r):
        for q in range(4):
            w_ready(r, q)
        project(r, 0, whole)
        y_start(r, 0)
        y_start(r, 1)
        project(r, 1, whole)
        y_start(r, 2)
        project(r, 2, whole)
        y_start(r, 3)
        project(r, 3, whole)

    def stage_b(r):
        up = p_out[r, 1, lo, :].astype(jnp.float32) + y_got(r, 0)
        p_out[r, 1, lo, :] = up.astype(jnp.bfloat16)
        y_start(r, 4)
        down = p_out[r, 2, hi, :].astype(jnp.float32) + y_got(r, 1)
        p_out[r, 2, hi, :] = down.astype(jnp.bfloat16)
        y_start(r, 5)

    def y_sum(r, half):
        slots = (3, 4) if half is lo else (2, 5)
        return p_out[r, 3, half, :].astype(jnp.float32) + y_got(r, slots[0]) + y_got(r, slots[1])

    def piece(p):
        return pl.ds(p * ROWS, ROWS)

    def cw(part, u):
        return range(PIECES - CCW[part][u])

    def ccw(part, u):
        return range(PIECES - CCW[part][u], PIECES)

    def each_place(act):
        for zi in range(4):
            for part in range(len(CCW)):

                @pl.when(jnp.logical_and(z == zi, z_lo // 2 == part))
                def _():
                    act(zi, part)

    def za_copy(r, way, p):
        return pltpu.make_async_remote_copy(
            src_ref=z_out.at[r, piece(p), :],
            dst_ref=za_in.at[way, p],
            send_sem=za_send.at[way, p],
            recv_sem=za_recv.at[way, p],
            device_id=dev(1 if way == 0 else 3, 0),
            device_id_type=MESH,
        )

    def zd_copy(r, way, p):
        return pltpu.make_async_remote_copy(
            src_ref=z_out.at[r, piece(p), :],
            dst_ref=zd_in.at[way, p],
            send_sem=zd_send.at[way, p],
            recv_sem=zd_recv.at[way, p],
            device_id=dev(1 if way == 0 else 3, 0),
            device_id_type=MESH,
        )

    def step_of(zi, u):
        return ORDER[zi].index(u % 4)

    def direct(zi, part, r, pieces):
        u = ORDER[zi][r]
        role = (u - zi) % 4
        for p in pieces:
            if role == 2 and p in cw(part, u):
                za_copy(r, 0, p).start()
            elif role == 2:
                za_copy(r, 1, p).start()
            elif role == 1 and p in ccw(part, u):
                zd_copy(r, 0, p).start()
            elif role == 3 and p in cw(part, u):
                zd_copy(r, 1, p).start()

    def y_done(r):
        for half, pieces in ((lo, (0, 1)), (hi, (2, 3))):
            z_out[r, half, :] = y_sum(r, half).astype(jnp.bfloat16)

            def act(zi, part):
                if (zi, r) != (3, 2):
                    direct(zi, part, r, pieces)

            each_place(act)

    def add_on(zi, way, p):
        r = step_of(zi, zi + 1 if way == 0 else zi - 1)
        za_copy(r, way, p).wait_recv()
        both = z_out[r, piece(p), :].astype(jnp.float32) + za_in[way, p].astype(jnp.float32)
        z_out[r, piece(p), :] = both.astype(jnp.bfloat16)
        zd_copy(r, way, p).start()

    @pl.when(jnp.logical_not(prompt))
    def _():
        hear(0)
        tell(1)
        hear(1)
        tell(2)

    first_stage()
    stage_b(0)
    stage(1)
    hear(2)
    y_done(0)
    stage_b(1)
    stage(2)
    y_done(1)
    stage_b(2)
    stage(3)
    y_done(2)
    stage_b(3)
    own[lo, :] = y_sum(3, lo)
    own[hi, :] = y_sum(3, hi)

    def relay_sums(zi, part):
        onward = [(0, p) for p in cw(part, (zi + 1) % 4)]
        back = [(1, p) for p in ccw(part, (zi + 3) % 4)]
        first, then = (onward, back) if zi == 3 else (back, onward)
        if zi == 2:
            for i in range(PIECES):
                for way, p in first[i : i + 1] + then[i : i + 1]:
                    add_on(zi, way, p)
        else:
            for way, p in first:
                add_on(zi, way, p)
            if zi == 3:
                direct(3, part, 2, range(PIECES))
            for way, p in then:
                add_on(zi, way, p)

    each_place(relay_sums)

    for p in range(PIECES):
        zd_copy(3, 0, p).wait_recv()
        zd_copy(3, 1, p).wait_recv()
        total = own[piece(p), :] + zd_in[0, p].astype(jnp.float32)
        out_ref[piece(p), :] = (total + zd_in[1, p].astype(jnp.float32)).astype(jnp.bfloat16)

    for k in range(1, BACK + 1):

        @pl.when(c + k < n_ctx)
        def _():
            doc_out(k).wait_send()
            kv_out(k).wait_send()

        @pl.when(c >= k)
        def _():
            forward(k, core).wait_send()

    a_copy(core, lo).wait_send()
    a_copy(core, hi).wait_send()
    for r in range(4):
        for q in range(4):
            w_cross(r, q).wait_send()
        for slot in range(6):
            y_copy(r, slot, y_src(r, slot)).wait_send()
    def sent(zi, part):
        for p in cw(part, (zi + 2) % 4):
            za_copy(0, 0, p).wait_send()
        for p in ccw(part, (zi + 2) % 4):
            za_copy(0, 1, p).wait_send()

    each_place(sent)

    for p in range(PIECES):
        zd_copy(0, 0, p).wait_send()
        zd_copy(0, 1, p).wait_send()


def solution(mesh):
    n_ctx = mesh.shape["context"]

    def body(query_rows, key_rows, value_rows, doc_ids, out_weight):
        dma = pltpu.SemaphoreType.DMA
        bf16, f32 = jnp.bfloat16, jnp.float32
        vmem = pl.BlockSpec(memory_space=pltpu.VMEM)
        hbm = pl.BlockSpec(memory_space=pltpu.HBM)

        def run(*refs):
            kernel(n_ctx, *refs)

        return pl.pallas_call(
            run,
            out_shape=jax.ShapeDtypeStruct((TOK, TOK), bf16),
            in_specs=[hbm, hbm, hbm, hbm, hbm],
            out_specs=vmem,
            scratch_shapes=[
                pltpu.VMEM((2, KEYS, HD), bf16),
                pltpu.VMEM((BLOCKS, 8, TOK), jnp.int32),
                pltpu.VMEM((TOK, TOK), jnp.int32),
                pltpu.VMEM((2, TOK, HD), f32),
                pltpu.VMEM((2, TOK, HD), f32),
                pltpu.VMEM((2, TOK, HD), f32),
                pltpu.VMEM((2, TOK, TOK), bf16),
                pltpu.VMEM((16, 2, TOK, TOK), bf16),
                pltpu.VMEM((4, 4, TOK, TOK), bf16),
                pltpu.VMEM((4, 6, HALF, TOK), bf16),
                pltpu.VMEM((4, TOK, TOK), bf16),
                pltpu.VMEM((2, PIECES, ROWS, TOK), bf16),
                pltpu.VMEM((2, PIECES, ROWS, TOK), bf16),
                pltpu.VMEM((TOK, TOK), bf16),
                pltpu.VMEM((1, TOK), jnp.int32),
                pltpu.VMEM((TOK, TOK), f32),
                pltpu.SemaphoreType.REGULAR((3, 2)),
                dma((4,)),
                dma((16,)),
                dma((16,)),
                dma((16,)),
                dma((BACK,)),
                dma((BACK,)),
                dma((BACK,)),
                dma((BACK,)),
                dma((BACK,)),
                dma((BACK,)),
                dma((2,)),
                dma((2,)),
                dma((4, 6)),
                dma((4, 6)),
                dma((2, PIECES)),
                dma((2, PIECES)),
                dma((2, PIECES)),
                dma((2, PIECES)),
            ],
            compiler_params=pltpu.CompilerParams(
                collective_id=0, has_side_effects=True, vmem_limit_bytes=60 * 2**20
            ),
        )(query_rows, key_rows, value_rows, doc_ids.reshape(1, TOK), out_weight)

    placed = (
        P("context", "tensor"),
        P("context", None),
        P("context", None),
        P("context"),
        P("tensor", None),
    )
    return jax.shard_map(
        body, mesh=mesh, in_specs=placed, out_specs=P("context", "tensor"), check_vma=False
    )
```

```python
import jax
import jax.numpy as jnp
from jax import lax
from jax.experimental import pallas as pl
from jax.experimental.pallas import tpu as pltpu
from jax.sharding import PartitionSpec as P

HD = 128
GROUP = 8
BACK = 4
TOK = 256
HALF = TOK // 2
NEG_BIG = -1e30
SCALE = HD**-0.5 * 1.4426950408889634
MESH = pl.DeviceIdType.MESH
OFFSETS = (2, 1, 3, 0)
ORDER = ((1, 2, 3, 0), (0, 3, 2, 1), (0, 1, 3, 2), (1, 0, 2, 3))
PIECES = 4
ROWS = TOK // PIECES
CCW = ((2, 3, 2, 1), (2, 2, 2, 1), (2, 2, 2, 2), (2, 2, 2, 2))
BLOCKS = BACK + 1
KEYS = BLOCKS * TOK


def kernel(
    n_ctx,
    q_ref,
    k_ref,
    v_ref,
    doc_ref,
    w_ref,
    out_ref,
    kv,
    docs,
    dq,
    m_buf,
    l_buf,
    n_buf,
    a_buf,
    w_buf,
    p_out,
    y_in,
    z_out,
    za_in,
    zd_in,
    q_buf,
    doc_buf,
    own,
    relay,
    loc_sem,
    w_sem,
    wx_send,
    wx_recv,
    kv_send,
    kv_recv,
    doc_send,
    doc_recv,
    fwd_send,
    fwd_recv,
    a_send,
    a_recv,
    y_send,
    y_recv,
    za_send,
    za_recv,
    zd_send,
    zd_recv,
):
    c = lax.axis_index("context")
    t = lax.axis_index("tensor")
    core = lax.rem(t, 2)
    y = lax.rem(t // 2, 4)
    z = t // 8
    other = 1 - core
    lo, hi, whole = pl.ds(0, HALF), pl.ds(HALF, HALF), pl.ds(0, TOK)

    def dev(dz, dy, same_core=True):
        who = core if same_core else other
        return {"tensor": (lax.rem(z + dz, 4) * 4 + lax.rem(y + dy, 4)) * 2 + who}

    x, z_lo = lax.rem(c, 4), c // 4

    def up(d):
        at = z_lo + d
        hi_part = lax.rem(z + at // 8, 4)
        return {"context": lax.rem(at, 8) * 4 + x, "tensor": (hi_part * 4 + y) * 2 + core}

    def down(d):
        at = z_lo + 8 - d
        hi_part = lax.rem(z + 3 + at // 8, 4)
        return {"context": lax.rem(at, 8) * 4 + x, "tensor": (hi_part * 4 + y) * 2 + core}

    def tell_one(i, way):
        d = (1, 2, 4)[i]
        where = up(d) if way == 1 else down(d)
        pl.semaphore_signal(relay.at[i, way], inc=1, device_id=where, device_id_type=MESH)

    def tell(i):
        tell_one(i, 1)
        tell_one(i, 0)

    def hear(i):
        pl.semaphore_wait(relay.at[i, 0], 1)
        pl.semaphore_wait(relay.at[i, 1], 1)

    prompt = z >= 2
    first_plane = jnp.logical_and(z == 0, z_lo == 0)

    barrier = pltpu.get_barrier_semaphore()

    @pl.when(jnp.logical_and(z_lo == 7, z < 3))
    def _():
        pl.semaphore_signal(barrier, inc=1, device_id=up(1), device_id_type=MESH)

    @pl.when(z_lo == 0)
    def _():
        pl.semaphore_signal(barrier, inc=1, device_id=down(1), device_id_type=MESH)

    for where in (dev(0, 0, False), dev(0, 1), dev(0, 3)):
        pl.semaphore_signal(barrier, inc=1, device_id=where, device_id_type=MESH)
    for k in range(1, BACK + 1):

        @pl.when(c + k < n_ctx)
        def _():
            pl.semaphore_signal(
                barrier, inc=1, device_id={"context": c + k}, device_id_type=MESH
            )

        @pl.when(c >= k)
        def _():
            pl.semaphore_signal(
                barrier, inc=1, device_id={"context": c - k}, device_id_type=MESH
            )

    head = pl.multiple_of((t // 4) * HD, HD)
    k_copy = pltpu.make_async_copy(
        k_ref.at[:, pl.ds(head, HD)], kv.at[0, pl.ds(0, TOK), :], loc_sem.at[0]
    )
    v_copy = pltpu.make_async_copy(
        v_ref.at[:, pl.ds(head, HD)], kv.at[1, pl.ds(0, TOK), :], loc_sem.at[1]
    )
    q_copy = pltpu.make_async_copy(q_ref, q_buf, loc_sem.at[2])
    doc_copy = pltpu.make_async_copy(doc_ref, doc_buf, loc_sem.at[3])
    doc_copy.start()
    k_copy.start()
    q_copy.start()
    v_copy.start()

    def columns(r, q, who):
        u = ORDER[3][r]
        for zi in range(3):
            u = jnp.where(z == zi, ORDER[zi][r], u)
        j = u * 4 + lax.rem(y + OFFSETS[q], 4)
        return pl.ds(pl.multiple_of((j * 2 + who) * TOK, TOK), TOK)

    def w_local(r, q):
        i = r * 4 + q
        return pltpu.make_async_copy(
            w_ref.at[:, columns(r, q, core)], w_buf.at[i, core], w_sem.at[i]
        )

    def w_cross(r, q):
        i = r * 4 + q
        return pltpu.make_async_remote_copy(
            src_ref=w_ref.at[:, columns(r, q, other)],
            dst_ref=w_buf.at[i, core],
            send_sem=wx_send.at[i],
            recv_sem=wx_recv.at[i],
            device_id=dev(0, 0, False),
            device_id_type=MESH,
        )

    def w_cross_in(r, q):
        i = r * 4 + q
        return pltpu.make_async_remote_copy(
            src_ref=w_ref.at[:, columns(r, q, other)],
            dst_ref=w_buf.at[i, other],
            send_sem=wx_send.at[i],
            recv_sem=wx_recv.at[i],
            device_id=dev(0, 0, False),
            device_id_type=MESH,
        )

    for r in range(4):
        for q in range(4):
            w_local(r, q).start()

    doc_copy.wait()
    row = doc_buf[...]
    docs[0] = jnp.broadcast_to(row, (8, TOK))
    dq[...] = jnp.broadcast_to(row, (TOK, TOK)).T
    for k in range(1, BACK + 1):

        @pl.when(c < k)
        def _():
            kv[:, pl.ds(k * TOK, TOK), :] = jnp.zeros((2, TOK, HD), jnp.bfloat16)
            docs[k] = jnp.full((8, TOK), -1, jnp.int32)

    def absorb(k, half):
        span = pl.ds(k * TOK, TOK)
        keys, values = kv[0, span, :], kv[1, span, :]
        mask = dq[half, :] == docs[k, 0:1, :]
        if k == 0:
            first = 0 if half is lo else HALF
            i = lax.broadcasted_iota(jnp.int32, (HALF, TOK), 0) + first
            j = lax.broadcasted_iota(jnp.int32, (HALF, TOK), 1)
            mask = mask & (j <= i)
        for h in range(2):
            s = lax.dot_general(
                q_buf[half, pl.ds(h * HD, HD)],
                keys,
                (((1,), (1,)), ((), ())),
                preferred_element_type=jnp.float32,
            )
            s = jnp.where(mask, s * SCALE, NEG_BIG)
            top = jnp.broadcast_to(jnp.max(s, axis=-1, keepdims=True), (HALF, HD))
            if k > 0:
                before = m_buf[h, half, :]
                top = jnp.maximum(before, top)
                keep = jnp.exp2(before - top)
            e = jnp.exp2(s - jnp.concatenate([top, top], axis=1))
            total = jnp.broadcast_to(jnp.sum(e, axis=-1, keepdims=True), (HALF, HD))
            numer = jnp.dot(e.astype(jnp.bfloat16), values, preferred_element_type=jnp.float32)
            if k > 0:
                total = total + keep * l_buf[h, half, :]
                numer = numer + keep * n_buf[h, half, :]
            if k == BACK:
                a_buf[core, half, pl.ds(h * HD, HD)] = (numer / total).astype(jnp.bfloat16)
            else:
                m_buf[h, half, :] = top
                l_buf[h, half, :] = total
                n_buf[h, half, :] = numer

    k_copy.wait()
    q_copy.wait()
    v_copy.wait()
    absorb(0, lo)
    absorb(0, hi)
    partners = 3 + jnp.minimum(c, BACK) + jnp.minimum(n_ctx - 1 - c, BACK)
    partners = partners + jnp.where(jnp.logical_and(z_lo == 0, z > 0), 1, 0)
    partners = partners + jnp.where(z_lo == 7, 1, 0)
    pl.semaphore_wait(barrier, partners)

    @pl.when(jnp.logical_not(first_plane))
    def _():
        tell(0)

    def kv_out(k):
        return pltpu.make_async_remote_copy(
            src_ref=kv.at[core, pl.ds(0, TOK), :],
            dst_ref=kv.at[core, pl.ds(k * TOK, TOK), :],
            send_sem=kv_send.at[k - 1],
            recv_sem=kv_recv.at[k - 1],
            device_id={"context": c + k},
            device_id_type=MESH,
        )

    def doc_out(k):
        return pltpu.make_async_remote_copy(
            src_ref=docs.at[0],
            dst_ref=docs.at[k],
            send_sem=doc_send.at[k - 1],
            recv_sem=doc_recv.at[k - 1],
            device_id={"context": c + k},
            device_id_type=MESH,
        )

    def forward(k, who):
        return pltpu.make_async_remote_copy(
            src_ref=kv.at[who, pl.ds(k * TOK, TOK), :],
            dst_ref=kv.at[who, pl.ds(k * TOK, TOK), :],
            send_sem=fwd_send.at[k - 1],
            recv_sem=fwd_recv.at[k - 1],
            device_id=dev(0, 0, False),
            device_id_type=MESH,
        )

    for k in range(1, BACK + 1):

        @pl.when(c + k < n_ctx)
        def _():
            doc_out(k).start()
            kv_out(k).start()

    for q in range(4):
        w_cross(0, q).start()

    for k in range(1, BACK + 1):

        @pl.when(c >= k)
        def _():
            kv_out(k).wait_recv()
            forward(k, core).start()

        if k == 3:

            @pl.when(prompt)
            def _():
                hear(0)
                tell(1)

        if k >= 2:

            @pl.when(c >= k - 1)
            def _():
                forward(k - 1, other).wait_recv()
                doc_out(k - 1).wait_recv()

            absorb(k - 1, lo)
            absorb(k - 1, hi)

    for r in range(1, 4):
        for q in range(4):
            w_cross(r, q).start()

    @pl.when(prompt)
    def _():
        hear(1)
        tell(2)

    @pl.when(c >= BACK)
    def _():
        forward(BACK, other).wait_recv()
        doc_out(BACK).wait_recv()

    def a_copy(who, half):
        n = 0 if half is lo else 1
        return pltpu.make_async_remote_copy(
            src_ref=a_buf.at[who, half, :],
            dst_ref=a_buf.at[who, half, :],
            send_sem=a_send.at[n],
            recv_sem=a_recv.at[n],
            device_id=dev(0, 0, False),
            device_id_type=MESH,
        )

    for half in (lo, hi):
        absorb(BACK, half)
        a_copy(core, half).start()

    def w_ready(r, q):
        w_local(r, q).wait()
        w_cross_in(r, q).wait_recv()

    def project(r, q, rows):
        i = r * 4 + q
        p = jnp.dot(a_buf[0, rows, :], w_buf[i, 0], preferred_element_type=jnp.float32)
        p = p + jnp.dot(a_buf[1, rows, :], w_buf[i, 1], preferred_element_type=jnp.float32)
        p_out[r, q, rows, :] = p.astype(jnp.bfloat16)

    def y_copy(r, slot, src):
        return pltpu.make_async_remote_copy(
            src_ref=src,
            dst_ref=y_in.at[r, slot],
            send_sem=y_send.at[r, slot],
            recv_sem=y_recv.at[r, slot],
            device_id=dev(0, 1 if slot % 2 == 0 else 3),
            device_id_type=MESH,
        )

    def y_src(r, slot):
        q, half = ((0, lo), (0, hi), (1, hi), (2, lo), (1, lo), (2, hi))[slot]
        return p_out.at[r, q, half, :]

    def y_start(r, slot):
        y_copy(r, slot, y_src(r, slot)).start()

    def y_got(r, slot):
        y_copy(r, slot, y_src(r, slot)).wait_recv()
        return y_in[r, slot].astype(jnp.float32)

    def first_stage():
        for q in range(4):
            w_ready(0, q)
        for half, (slot_a, slot_d, q_d, q_b) in ((lo, (0, 3, 2, 1)), (hi, (1, 2, 1, 2))):
            a_copy(other, half).wait_recv()
            project(0, 0, half)
            y_start(0, slot_a)
            project(0, q_d, half)
            y_start(0, slot_d)
            project(0, q_b, half)
        project(0, 3, whole)

    def stage(r):
        for q in range(4):
            w_ready(r, q)
        project(r, 0, whole)
        y_start(r, 0)
        y_start(r, 1)
        project(r, 1, whole)
        y_start(r, 2)
        project(r, 2, whole)
        y_start(r, 3)
        project(r, 3, whole)

    def stage_b(r):
        up = p_out[r, 1, lo, :].astype(jnp.float32) + y_got(r, 0)
        p_out[r, 1, lo, :] = up.astype(jnp.bfloat16)
        y_start(r, 4)
        down = p_out[r, 2, hi, :].astype(jnp.float32) + y_got(r, 1)
        p_out[r, 2, hi, :] = down.astype(jnp.bfloat16)
        y_start(r, 5)

    def y_sum(r, half):
        slots = (3, 4) if half is lo else (2, 5)
        return p_out[r, 3, half, :].astype(jnp.float32) + y_got(r, slots[0]) + y_got(r, slots[1])

    def piece(p):
        return pl.ds(p * ROWS, ROWS)

    def cw(part, u):
        return range(PIECES - CCW[part][u])

    def ccw(part, u):
        return range(PIECES - CCW[part][u], PIECES)

    def each_place(act):
        for zi in range(4):
            for part in range(len(CCW)):

                @pl.when(jnp.logical_and(z == zi, z_lo // 2 == part))
                def _():
                    act(zi, part)

    def za_copy(r, way, p):
        return pltpu.make_async_remote_copy(
            src_ref=z_out.at[r, piece(p), :],
            dst_ref=za_in.at[way, p],
            send_sem=za_send.at[way, p],
            recv_sem=za_recv.at[way, p],
            device_id=dev(1 if way == 0 else 3, 0),
            device_id_type=MESH,
        )

    def zd_copy(r, way, p):
        return pltpu.make_async_remote_copy(
            src_ref=z_out.at[r, piece(p), :],
            dst_ref=zd_in.at[way, p],
            send_sem=zd_send.at[way, p],
            recv_sem=zd_recv.at[way, p],
            device_id=dev(1 if way == 0 else 3, 0),
            device_id_type=MESH,
        )

    def step_of(zi, u):
        return ORDER[zi].index(u % 4)

    def direct(zi, part, r, pieces):
        u = ORDER[zi][r]
        role = (u - zi) % 4
        for p in pieces:
            if role == 2 and p in cw(part, u):
                za_copy(r, 0, p).start()
            elif role == 2:
                za_copy(r, 1, p).start()
            elif role == 1 and p in ccw(part, u):
                zd_copy(r, 0, p).start()
            elif role == 3 and p in cw(part, u):
                zd_copy(r, 1, p).start()

    def y_done(r):
        for half, pieces in ((lo, range(PIECES // 2)), (hi, range(PIECES // 2, PIECES))):
            z_out[r, half, :] = y_sum(r, half).astype(jnp.bfloat16)

            def act(zi, part):
                if (zi, r) != (3, 2):
                    direct(zi, part, r, pieces)

            each_place(act)

    def add_on(zi, way, p):
        r = step_of(zi, zi + 1 if way == 0 else zi - 1)
        za_copy(r, way, p).wait_recv()
        both = z_out[r, piece(p), :].astype(jnp.float32) + za_in[way, p].astype(jnp.float32)
        z_out[r, piece(p), :] = both.astype(jnp.bfloat16)
        zd_copy(r, way, p).start()

    @pl.when(jnp.logical_not(prompt))
    def _():
        hear(0)

        @pl.when(first_plane)
        def _():
            tell(0)

        tell(1)
        hear(1)
        tell(2)

    first_stage()
    stage_b(0)
    stage(1)
    hear(2)
    y_done(0)
    stage_b(1)
    stage(2)
    y_done(1)
    stage_b(2)
    stage(3)
    y_done(2)
    stage_b(3)
    own[lo, :] = y_sum(3, lo)
    own[hi, :] = y_sum(3, hi)

    def relay_sums(zi, part):
        onward = [(0, p) for p in cw(part, (zi + 1) % 4)]
        back = [(1, p) for p in ccw(part, (zi + 3) % 4)]
        first, then = (onward, back) if zi == 3 else (back, onward)
        if zi == 2:
            for i in range(PIECES):
                for way, p in first[i : i + 1] + then[i : i + 1]:
                    add_on(zi, way, p)
        else:
            for way, p in first:
                add_on(zi, way, p)
            if zi == 3:
                direct(3, part, 2, range(PIECES))
            for way, p in then:
                add_on(zi, way, p)

    each_place(relay_sums)

    for p in range(PIECES):
        zd_copy(3, 0, p).wait_recv()
        zd_copy(3, 1, p).wait_recv()
        total = own[piece(p), :] + zd_in[0, p].astype(jnp.float32)
        out_ref[piece(p), :] = (total + zd_in[1, p].astype(jnp.float32)).astype(jnp.bfloat16)

    for k in range(1, BACK + 1):

        @pl.when(c + k < n_ctx)
        def _():
            doc_out(k).wait_send()
            kv_out(k).wait_send()

        @pl.when(c >= k)
        def _():
            forward(k, core).wait_send()

    a_copy(core, lo).wait_send()
    a_copy(core, hi).wait_send()
    for r in range(4):
        for q in range(4):
            w_cross(r, q).wait_send()
        for slot in range(6):
            y_copy(r, slot, y_src(r, slot)).wait_send()
    def sent(zi, part):
        for p in cw(part, (zi + 2) % 4):
            za_copy(0, 0, p).wait_send()
        for p in ccw(part, (zi + 2) % 4):
            za_copy(0, 1, p).wait_send()

    each_place(sent)

    for p in range(PIECES):
        zd_copy(0, 0, p).wait_send()
        zd_copy(0, 1, p).wait_send()


def solution(mesh):
    n_ctx = mesh.shape["context"]

    def body(query_rows, key_rows, value_rows, doc_ids, out_weight):
        dma = pltpu.SemaphoreType.DMA
        bf16, f32 = jnp.bfloat16, jnp.float32
        vmem = pl.BlockSpec(memory_space=pltpu.VMEM)
        hbm = pl.BlockSpec(memory_space=pltpu.HBM)

        def run(*refs):
            kernel(n_ctx, *refs)

        return pl.pallas_call(
            run,
            out_shape=jax.ShapeDtypeStruct((TOK, TOK), bf16),
            in_specs=[hbm, hbm, hbm, hbm, hbm],
            out_specs=vmem,
            scratch_shapes=[
                pltpu.VMEM((2, KEYS, HD), bf16),
                pltpu.VMEM((BLOCKS, 8, TOK), jnp.int32),
                pltpu.VMEM((TOK, TOK), jnp.int32),
                pltpu.VMEM((2, TOK, HD), f32),
                pltpu.VMEM((2, TOK, HD), f32),
                pltpu.VMEM((2, TOK, HD), f32),
                pltpu.VMEM((2, TOK, TOK), bf16),
                pltpu.VMEM((16, 2, TOK, TOK), bf16),
                pltpu.VMEM((4, 4, TOK, TOK), bf16),
                pltpu.VMEM((4, 6, HALF, TOK), bf16),
                pltpu.VMEM((4, TOK, TOK), bf16),
                pltpu.VMEM((2, PIECES, ROWS, TOK), bf16),
                pltpu.VMEM((2, PIECES, ROWS, TOK), bf16),
                pltpu.VMEM((TOK, TOK), bf16),
                pltpu.VMEM((1, TOK), jnp.int32),
                pltpu.VMEM((TOK, TOK), f32),
                pltpu.SemaphoreType.REGULAR((3, 2)),
                dma((4,)),
                dma((16,)),
                dma((16,)),
                dma((16,)),
                dma((BACK,)),
                dma((BACK,)),
                dma((BACK,)),
                dma((BACK,)),
                dma((BACK,)),
                dma((BACK,)),
                dma((2,)),
                dma((2,)),
                dma((4, 6)),
                dma((4, 6)),
                dma((2, PIECES)),
                dma((2, PIECES)),
                dma((2, PIECES)),
                dma((2, PIECES)),
            ],
            compiler_params=pltpu.CompilerParams(
                collective_id=0, has_side_effects=True, vmem_limit_bytes=60 * 2**20
            ),
        )(query_rows, key_rows, value_rows, doc_ids.reshape(1, TOK), out_weight)

    placed = (
        P("context", "tensor"),
        P("context", None),
        P("context", None),
        P("context"),
        P("tensor", None),
    )
    return jax.shard_map(
        body, mesh=mesh, in_specs=placed, out_specs=P("context", "tensor"), check_vma=False
    )
```

```python
import jax
import jax.numpy as jnp
from jax import lax
from jax.experimental import pallas as pl
from jax.experimental.pallas import tpu as pltpu
from jax.sharding import PartitionSpec as P

HD = 128
GROUP = 8
BACK = 4
TOK = 256
HALF = TOK // 2
NEG_BIG = -1e30
SCALE = HD**-0.5 * 1.4426950408889634
MESH = pl.DeviceIdType.MESH
OFFSETS = (2, 1, 3, 0)
ORDER = ((1, 2, 3, 0), (0, 3, 2, 1), (0, 1, 3, 2), (1, 0, 2, 3))
PIECES = 4
ROWS = TOK // PIECES
CCW = ((2, 3, 2, 1), (2, 2, 2, 1), (2, 2, 2, 2), (2, 2, 2, 2))
BLOCKS = BACK + 1
KEYS = BLOCKS * TOK


def kernel(
    n_ctx,
    q_ref,
    k_ref,
    v_ref,
    doc_ref,
    w_ref,
    out_ref,
    kv,
    docs,
    dq,
    m_buf,
    l_buf,
    n_buf,
    a_buf,
    w_buf,
    p_out,
    y_in,
    z_out,
    za_in,
    zd_in,
    q_buf,
    doc_buf,
    own,
    relay,
    loc_sem,
    w_sem,
    wx_send,
    wx_recv,
    kv_send,
    kv_recv,
    doc_send,
    doc_recv,
    fwd_send,
    fwd_recv,
    a_send,
    a_recv,
    y_send,
    y_recv,
    za_send,
    za_recv,
    zd_send,
    zd_recv,
):
    c = lax.axis_index("context")
    t = lax.axis_index("tensor")
    core = lax.rem(t, 2)
    y = lax.rem(t // 2, 4)
    z = t // 8
    other = 1 - core
    lo, hi, whole = pl.ds(0, HALF), pl.ds(HALF, HALF), pl.ds(0, TOK)

    def dev(dz, dy, same_core=True):
        who = core if same_core else other
        return {"tensor": (lax.rem(z + dz, 4) * 4 + lax.rem(y + dy, 4)) * 2 + who}

    x, z_lo = lax.rem(c, 4), c // 4

    def up(d):
        at = z_lo + d
        hi_part = lax.rem(z + at // 8, 4)
        return {"context": lax.rem(at, 8) * 4 + x, "tensor": (hi_part * 4 + y) * 2 + core}

    def down(d):
        at = z_lo + 8 - d
        hi_part = lax.rem(z + 3 + at // 8, 4)
        return {"context": lax.rem(at, 8) * 4 + x, "tensor": (hi_part * 4 + y) * 2 + core}

    def tell_one(i, way):
        d = (1, 2, 4)[i]
        where = up(d) if way == 1 else down(d)
        pl.semaphore_signal(relay.at[i, way], inc=1, device_id=where, device_id_type=MESH)

    def tell(i):
        tell_one(i, 1)
        tell_one(i, 0)

    def hear(i):
        pl.semaphore_wait(relay.at[i, 0], 1)
        pl.semaphore_wait(relay.at[i, 1], 1)

    prompt = z >= 2
    first_plane = jnp.logical_and(z == 0, z_lo == 0)

    barrier = pltpu.get_barrier_semaphore()

    @pl.when(jnp.logical_and(z_lo == 7, z < 3))
    def _():
        pl.semaphore_signal(barrier, inc=1, device_id=up(1), device_id_type=MESH)

    @pl.when(z_lo == 0)
    def _():
        pl.semaphore_signal(barrier, inc=1, device_id=down(1), device_id_type=MESH)

    for where in (dev(0, 0, False), dev(0, 1), dev(0, 3)):
        pl.semaphore_signal(barrier, inc=1, device_id=where, device_id_type=MESH)
    for k in range(1, BACK + 1):

        @pl.when(c + k < n_ctx)
        def _():
            pl.semaphore_signal(
                barrier, inc=1, device_id={"context": c + k}, device_id_type=MESH
            )

        @pl.when(c >= k)
        def _():
            pl.semaphore_signal(
                barrier, inc=1, device_id={"context": c - k}, device_id_type=MESH
            )

    head = pl.multiple_of((t // 4) * HD, HD)
    k_copy = pltpu.make_async_copy(
        k_ref.at[:, pl.ds(head, HD)], kv.at[0, pl.ds(0, TOK), :], loc_sem.at[0]
    )
    v_copy = pltpu.make_async_copy(
        v_ref.at[:, pl.ds(head, HD)], kv.at[1, pl.ds(0, TOK), :], loc_sem.at[1]
    )
    q_copy = pltpu.make_async_copy(q_ref, q_buf, loc_sem.at[2])
    doc_copy = pltpu.make_async_copy(doc_ref, doc_buf, loc_sem.at[3])
    doc_copy.start()
    k_copy.start()
    q_copy.start()
    v_copy.start()

    def columns(r, q, who):
        u = ORDER[3][r]
        for zi in range(3):
            u = jnp.where(z == zi, ORDER[zi][r], u)
        j = u * 4 + lax.rem(y + OFFSETS[q], 4)
        return pl.ds(pl.multiple_of((j * 2 + who) * TOK, TOK), TOK)

    def w_local(r, q):
        i = r * 4 + q
        return pltpu.make_async_copy(
            w_ref.at[:, columns(r, q, core)], w_buf.at[i, core], w_sem.at[i]
        )

    def w_cross(r, q):
        i = r * 4 + q
        return pltpu.make_async_remote_copy(
            src_ref=w_ref.at[:, columns(r, q, other)],
            dst_ref=w_buf.at[i, core],
            send_sem=wx_send.at[i],
            recv_sem=wx_recv.at[i],
            device_id=dev(0, 0, False),
            device_id_type=MESH,
        )

    def w_cross_in(r, q):
        i = r * 4 + q
        return pltpu.make_async_remote_copy(
            src_ref=w_ref.at[:, columns(r, q, other)],
            dst_ref=w_buf.at[i, other],
            send_sem=wx_send.at[i],
            recv_sem=wx_recv.at[i],
            device_id=dev(0, 0, False),
            device_id_type=MESH,
        )

    for r in range(4):
        for q in range(4):
            w_local(r, q).start()

    doc_copy.wait()
    row = doc_buf[...]
    docs[0] = jnp.broadcast_to(row, (8, TOK))
    dq[...] = jnp.broadcast_to(row, (TOK, TOK)).T
    for k in range(1, BACK + 1):

        @pl.when(c < k)
        def _():
            kv[:, pl.ds(k * TOK, TOK), :] = jnp.zeros((2, TOK, HD), jnp.bfloat16)
            docs[k] = jnp.full((8, TOK), -1, jnp.int32)

    def absorb(k, half):
        span = pl.ds(k * TOK, TOK)
        keys, values = kv[0, span, :], kv[1, span, :]
        mask = dq[half, :] == docs[k, 0:1, :]
        if k == 0:
            first = 0 if half is lo else HALF
            i = lax.broadcasted_iota(jnp.int32, (HALF, TOK), 0) + first
            j = lax.broadcasted_iota(jnp.int32, (HALF, TOK), 1)
            mask = mask & (j <= i)
        for h in range(2):
            s = lax.dot_general(
                q_buf[half, pl.ds(h * HD, HD)],
                keys,
                (((1,), (1,)), ((), ())),
                preferred_element_type=jnp.float32,
            )
            s = jnp.where(mask, s * SCALE, NEG_BIG)
            top = jnp.broadcast_to(jnp.max(s, axis=-1, keepdims=True), (HALF, HD))
            if k > 0:
                before = m_buf[h, half, :]
                top = jnp.maximum(before, top)
                keep = jnp.exp2(before - top)
            e = jnp.exp2(s - jnp.concatenate([top, top], axis=1))
            total = jnp.broadcast_to(jnp.sum(e, axis=-1, keepdims=True), (HALF, HD))
            numer = jnp.dot(e.astype(jnp.bfloat16), values, preferred_element_type=jnp.float32)
            if k > 0:
                total = total + keep * l_buf[h, half, :]
                numer = numer + keep * n_buf[h, half, :]
            if k == BACK:
                a_buf[core, half, pl.ds(h * HD, HD)] = (numer / total).astype(jnp.bfloat16)
            else:
                m_buf[h, half, :] = top
                l_buf[h, half, :] = total
                n_buf[h, half, :] = numer

    k_copy.wait()
    q_copy.wait()
    v_copy.wait()
    absorb(0, lo)
    absorb(0, hi)
    partners = 3 + jnp.minimum(c, BACK) + jnp.minimum(n_ctx - 1 - c, BACK)
    partners = partners + jnp.where(jnp.logical_and(z_lo == 0, z > 0), 1, 0)
    partners = partners + jnp.where(z_lo == 7, 1, 0)
    pl.semaphore_wait(barrier, partners)

    @pl.when(jnp.logical_not(first_plane))
    def _():
        tell(0)

    def kv_out(k):
        return pltpu.make_async_remote_copy(
            src_ref=kv.at[core, pl.ds(0, TOK), :],
            dst_ref=kv.at[core, pl.ds(k * TOK, TOK), :],
            send_sem=kv_send.at[k - 1],
            recv_sem=kv_recv.at[k - 1],
            device_id={"context": c + k},
            device_id_type=MESH,
        )

    def doc_out(k):
        return pltpu.make_async_remote_copy(
            src_ref=docs.at[0],
            dst_ref=docs.at[k],
            send_sem=doc_send.at[k - 1],
            recv_sem=doc_recv.at[k - 1],
            device_id={"context": c + k},
            device_id_type=MESH,
        )

    def forward(k, who):
        return pltpu.make_async_remote_copy(
            src_ref=kv.at[who, pl.ds(k * TOK, TOK), :],
            dst_ref=kv.at[who, pl.ds(k * TOK, TOK), :],
            send_sem=fwd_send.at[k - 1],
            recv_sem=fwd_recv.at[k - 1],
            device_id=dev(0, 0, False),
            device_id_type=MESH,
        )

    for k in range(1, BACK + 1):

        @pl.when(c + k < n_ctx)
        def _():
            doc_out(k).start()
            kv_out(k).start()

    for q in range(4):
        w_cross(0, q).start()

    for k in range(1, BACK + 1):

        @pl.when(c >= k)
        def _():
            kv_out(k).wait_recv()
            forward(k, core).start()

        if k == 3:

            @pl.when(prompt)
            def _():
                hear(0)
                tell(1)

        if k >= 2:

            @pl.when(c >= k - 1)
            def _():
                forward(k - 1, other).wait_recv()
                doc_out(k - 1).wait_recv()

            absorb(k - 1, lo)
            absorb(k - 1, hi)

    for r in range(1, 4):
        for q in range(4):
            w_cross(r, q).start()

    @pl.when(prompt)
    def _():
        hear(1)
        tell(2)

    @pl.when(c >= BACK)
    def _():
        forward(BACK, other).wait_recv()
        doc_out(BACK).wait_recv()

    def a_copy(who, half):
        n = 0 if half is lo else 1
        return pltpu.make_async_remote_copy(
            src_ref=a_buf.at[who, half, :],
            dst_ref=a_buf.at[who, half, :],
            send_sem=a_send.at[n],
            recv_sem=a_recv.at[n],
            device_id=dev(0, 0, False),
            device_id_type=MESH,
        )

    for half in (lo, hi):
        absorb(BACK, half)
        a_copy(core, half).start()

    def w_ready(r, q):
        w_local(r, q).wait()
        w_cross_in(r, q).wait_recv()

    def project(r, q, rows):
        i = r * 4 + q
        p = jnp.dot(a_buf[0, rows, :], w_buf[i, 0], preferred_element_type=jnp.float32)
        p = p + jnp.dot(a_buf[1, rows, :], w_buf[i, 1], preferred_element_type=jnp.float32)
        p_out[r, q, rows, :] = p.astype(jnp.bfloat16)

    def y_copy(r, slot, src):
        return pltpu.make_async_remote_copy(
            src_ref=src,
            dst_ref=y_in.at[r, slot],
            send_sem=y_send.at[r, slot],
            recv_sem=y_recv.at[r, slot],
            device_id=dev(0, 1 if slot % 2 == 0 else 3),
            device_id_type=MESH,
        )

    def y_src(r, slot):
        q, half = ((0, lo), (0, hi), (1, hi), (2, lo), (1, lo), (2, hi))[slot]
        return p_out.at[r, q, half, :]

    def y_start(r, slot):
        y_copy(r, slot, y_src(r, slot)).start()

    def y_got(r, slot):
        y_copy(r, slot, y_src(r, slot)).wait_recv()
        return y_in[r, slot].astype(jnp.float32)

    def first_stage():
        for q in range(4):
            w_ready(0, q)
        for half, (slot_a, slot_d, q_d, q_b) in ((lo, (0, 3, 2, 1)), (hi, (1, 2, 1, 2))):
            a_copy(other, half).wait_recv()
            project(0, 0, half)
            y_start(0, slot_a)
            project(0, q_d, half)
            y_start(0, slot_d)
            project(0, q_b, half)
        project(0, 3, whole)

    def stage(r):
        for q in range(4):
            w_ready(r, q)
        project(r, 0, whole)
        y_start(r, 0)
        y_start(r, 1)
        project(r, 1, whole)
        y_start(r, 2)
        project(r, 2, whole)
        y_start(r, 3)
        project(r, 3, whole)

    def stage_b(r):
        up = p_out[r, 1, lo, :].astype(jnp.float32) + y_got(r, 0)
        p_out[r, 1, lo, :] = up.astype(jnp.bfloat16)
        y_start(r, 4)
        down = p_out[r, 2, hi, :].astype(jnp.float32) + y_got(r, 1)
        p_out[r, 2, hi, :] = down.astype(jnp.bfloat16)
        y_start(r, 5)

    def y_sum(r, half):
        slots = (3, 4) if half is lo else (2, 5)
        return p_out[r, 3, half, :].astype(jnp.float32) + y_got(r, slots[0]) + y_got(r, slots[1])

    def piece(p):
        return pl.ds(p * ROWS, ROWS)

    def cw(part, u):
        return range(PIECES - CCW[part][u])

    def ccw(part, u):
        return range(PIECES - CCW[part][u], PIECES)

    def each_place(act):
        for zi in range(4):
            for part in range(len(CCW)):

                @pl.when(jnp.logical_and(z == zi, z_lo // 2 == part))
                def _():
                    act(zi, part)

    def za_copy(r, way, p):
        return pltpu.make_async_remote_copy(
            src_ref=z_out.at[r, piece(p), :],
            dst_ref=za_in.at[way, p],
            send_sem=za_send.at[way, p],
            recv_sem=za_recv.at[way, p],
            device_id=dev(1 if way == 0 else 3, 0),
            device_id_type=MESH,
        )

    def zd_copy(r, way, p):
        return pltpu.make_async_remote_copy(
            src_ref=z_out.at[r, piece(p), :],
            dst_ref=zd_in.at[way, p],
            send_sem=zd_send.at[way, p],
            recv_sem=zd_recv.at[way, p],
            device_id=dev(1 if way == 0 else 3, 0),
            device_id_type=MESH,
        )

    def step_of(zi, u):
        return ORDER[zi].index(u % 4)

    def direct(zi, part, r, pieces):
        u = ORDER[zi][r]
        role = (u - zi) % 4
        for p in pieces:
            if role == 2 and p in cw(part, u):
                za_copy(r, 0, p).start()
            elif role == 2:
                za_copy(r, 1, p).start()
            elif role == 1 and p in ccw(part, u):
                zd_copy(r, 0, p).start()
            elif role == 3 and p in cw(part, u):
                zd_copy(r, 1, p).start()

    def y_done(r):
        for half, pieces in ((lo, range(PIECES // 2)), (hi, range(PIECES // 2, PIECES))):
            z_out[r, half, :] = y_sum(r, half).astype(jnp.bfloat16)

            def act(zi, part):
                if (zi, r) != (3, 2):
                    direct(zi, part, r, pieces)

            each_place(act)

    def add_on(zi, way, p):
        r = step_of(zi, zi + 1 if way == 0 else zi - 1)
        za_copy(r, way, p).wait_recv()
        both = z_out[r, piece(p), :].astype(jnp.float32) + za_in[way, p].astype(jnp.float32)
        z_out[r, piece(p), :] = both.astype(jnp.bfloat16)
        zd_copy(r, way, p).start()

    @pl.when(jnp.logical_not(prompt))
    def _():
        hear(0)

        @pl.when(first_plane)
        def _():
            tell(0)

        tell(1)
        hear(1)
        tell(2)

    first_stage()
    stage_b(0)
    stage(1)
    hear(2)
    y_done(0)
    stage_b(1)
    stage(2)
    y_done(1)
    stage_b(2)
    stage(3)
    y_done(2)
    stage_b(3)
    own[lo, :] = y_sum(3, lo)
    own[hi, :] = y_sum(3, hi)

    def relay_sums(zi, part):
        onward = [(0, p) for p in cw(part, (zi + 1) % 4)]
        back = [(1, p) for p in ccw(part, (zi + 3) % 4)]
        first, then = (onward, back) if zi == 3 else (back, onward)
        if zi == 2:
            for i in range(PIECES):
                for way, p in first[i : i + 1] + then[i : i + 1]:
                    add_on(zi, way, p)
        else:
            for way, p in first:
                add_on(zi, way, p)
            if zi == 3:
                direct(3, part, 2, range(PIECES))
            for way, p in then:
                add_on(zi, way, p)

    each_place(relay_sums)

    for p in range(PIECES):
        zd_copy(3, 0, p).wait_recv()
        zd_copy(3, 1, p).wait_recv()
        total = own[piece(p), :] + zd_in[0, p].astype(jnp.float32)
        out_ref[piece(p), :] = (total + zd_in[1, p].astype(jnp.float32)).astype(jnp.bfloat16)

    for k in range(1, BACK + 1):

        @pl.when(c + k < n_ctx)
        def _():
            doc_out(k).wait_send()
            kv_out(k).wait_send()

        @pl.when(c >= k)
        def _():
            forward(k, core).wait_send()

    a_copy(core, lo).wait_send()
    a_copy(core, hi).wait_send()
    for r in range(4):
        for q in range(4):
            w_cross(r, q).wait_send()
        for slot in range(6):
            y_copy(r, slot, y_src(r, slot)).wait_send()
    def sent(zi, part):
        for p in cw(part, (zi + 2) % 4):
            za_copy(0, 0, p).wait_send()
        for p in ccw(part, (zi + 2) % 4):
            za_copy(0, 1, p).wait_send()

    each_place(sent)

    for p in range(PIECES):
        zd_copy(0, 0, p).wait_send()
        zd_copy(0, 1, p).wait_send()


def solution(mesh):
    n_ctx = mesh.shape["context"]

    def body(query_rows, key_rows, value_rows, doc_ids, out_weight):
        dma = pltpu.SemaphoreType.DMA
        bf16, f32 = jnp.bfloat16, jnp.float32
        vmem = pl.BlockSpec(memory_space=pltpu.VMEM)
        hbm = pl.BlockSpec(memory_space=pltpu.HBM)

        def run(*refs):
            kernel(n_ctx, *refs)

        return pl.pallas_call(
            run,
            out_shape=jax.ShapeDtypeStruct((TOK, TOK), bf16),
            in_specs=[hbm, hbm, hbm, hbm, hbm],
            out_specs=vmem,
            scratch_shapes=[
                pltpu.VMEM((2, KEYS, HD), bf16),
                pltpu.VMEM((BLOCKS, 8, TOK), jnp.int32),
                pltpu.VMEM((TOK, TOK), jnp.int32),
                pltpu.VMEM((2, TOK, HD), f32),
                pltpu.VMEM((2, TOK, HD), f32),
                pltpu.VMEM((2, TOK, HD), f32),
                pltpu.VMEM((2, TOK, TOK), bf16),
                pltpu.VMEM((16, 2, TOK, TOK), bf16),
                pltpu.VMEM((4, 4, TOK, TOK), bf16),
                pltpu.VMEM((4, 6, HALF, TOK), bf16),
                pltpu.VMEM((4, TOK, TOK), bf16),
                pltpu.VMEM((2, PIECES, ROWS, TOK), bf16),
                pltpu.VMEM((2, PIECES, ROWS, TOK), bf16),
                pltpu.VMEM((TOK, TOK), bf16),
                pltpu.VMEM((1, TOK), jnp.int32),
                pltpu.VMEM((TOK, TOK), f32),
                pltpu.SemaphoreType.REGULAR((3, 2)),
                dma((4,)),
                dma((16,)),
                dma((16,)),
                dma((16,)),
                dma((BACK,)),
                dma((BACK,)),
                dma((BACK,)),
                dma((BACK,)),
                dma((BACK,)),
                dma((BACK,)),
                dma((2,)),
                dma((2,)),
                dma((4, 6)),
                dma((4, 6)),
                dma((2, PIECES)),
                dma((2, PIECES)),
                dma((2, PIECES)),
                dma((2, PIECES)),
            ],
            compiler_params=pltpu.CompilerParams(
                collective_id=0, has_side_effects=True, vmem_limit_bytes=52 * 2**20
            ),
        )(query_rows, key_rows, value_rows, doc_ids.reshape(1, TOK), out_weight)

    placed = (
        P("context", "tensor"),
        P("context", None),
        P("context", None),
        P("context"),
        P("tensor", None),
    )
    return jax.shard_map(
        body, mesh=mesh, in_specs=placed, out_specs=P("context", "tensor"), check_vma=False
    )
```
